1024 devices in a mesh: group: 16 (over y, x_hi), expert: 32 (over z, core), dp: 2 (over x_lo).
Axes of the slice: x: 4 (x_hi: 2, x_lo: 2; x = x_hi * 2 + x_lo), y: 8, z: 16, core: 2. Of those that a mesh axis runs over, the one named last changes fastest.
Arguments:
- tokens: bfloat16 [64, 64, 7168], P(('expert', 'dp'), 'group'), may hold values from -6 to 6
- expert_ids: int32 [64, 64, 8], P(('expert', 'dp')), may hold values from 0 to 255, as said below
- gate_codes: int32 [64, 64, 8], P(('expert', 'dp')), may hold values from 1 to 1023
- w_gate: bfloat16 [32, 7168, 2048], P('expert', None, 'group'), may hold values from -0.0625 to 0.0625
- w_up: bfloat16 [32, 7168, 2048], P('expert', None, 'group'), may hold values from -0.0625 to 0.0625
- w_down: bfloat16 [32, 2048, 7168], P('expert', 'group'), may hold values from -0.125 to 0.125
Outputs:
- mixed: bfloat16 [64, 64, 7168], P(('expert', 'dp'), 'group')
The draws below stay inside these ranges and needn't reach their ends.
Inputs may be any that keep to these rules, and one draw needn't show every extreme that they name: `expert_ids`: each token names 8 different experts, all within at most 4 of the 8 groups of 32 consecutive ids. In every set (one index of the first dimension), each expert below 32 is named by at most 4 tokens, and some expert by exactly 4; a token names at most 4 experts below 32.
All inputs are finite; a program needn't handle non-finite values.
Results may differ from the reference program's by a relative error of at most 0.015.
Values may be sent and summed in bfloat16 or wider, within the bound.
No kernel may reach another device: no remote copies, remote signals or barrier semaphores. Data moves between devices by JAX's collectives and lax.ppermute only.
A program may use at most 64 MiB of HBM per device.

```python
import jax
import jax.numpy as jnp
from jax import lax

D = 7168
FF = 2048
TOP = 8
NODE_GROUPS = 8
MAX_NODES = 4
CAPG = 4
EXPERTS = 32
SET_TOK = 64
SETS = 64
N_GROUP = 16


def draw_others(key, count):
    keys = jax.random.split(key, 3)
    groups = jax.random.permutation(keys[0], NODE_GROUPS - 1)[:MAX_NODES] + 1
    fewer = jax.random.permutation(keys[1], (MAX_NODES - 1) * EXPERTS)[:TOP]
    wider = jax.random.permutation(keys[2], MAX_NODES * EXPERTS)[:TOP]
    local = jnp.where(count > 0, fewer, wider)
    return groups[local // EXPERTS] * EXPERTS + local % EXPERTS


def shuffle_row(key, row):
    return jax.random.permutation(key, row)


def draw_one_set(key):
    keys = jax.random.split(key, 6)
    spacing = SET_TOK // CAPG
    offsets = jax.random.permutation(keys[0], SET_TOK)[:EXPERTS]
    order = jax.random.permutation(keys[1], SET_TOK)
    slot_index = jnp.arange(CAPG)
    slot_token = order[(offsets[:, None] + spacing * slot_index[None, :]) % SET_TOK]
    live = jax.random.randint(keys[2], (EXPERTS, CAPG), 0, 2)
    chosen = jax.random.randint(keys[3], (), 0, EXPERTS)
    live = jnp.where(jnp.arange(EXPERTS)[:, None] == chosen, 1, live)
    token_index = jnp.arange(SET_TOK)
    member = jnp.sum(jnp.where(slot_token[None, :, :] == token_index[:, None, None], live[None, :, :], 0), axis=2)
    count = jnp.sum(member, axis=1)
    position = jnp.cumsum(member, axis=1) - member
    picks = jnp.arange(TOP)
    window_ids = jnp.sum(jnp.where((member[:, :, None] == 1) & (position[:, :, None] == picks[None, None, :]), jnp.arange(EXPERTS)[None, :, None], 0), axis=1)
    others = jax.vmap(draw_others)(jax.random.split(keys[4], SET_TOK), count)
    offset_pick = jnp.clip(picks[None, :] - count[:, None], 0, TOP - 1)
    other_ids = jnp.take_along_axis(others, offset_pick, axis=1)
    chosen_ids = jnp.where(picks[None, :] < count[:, None], window_ids, other_ids)
    return jax.vmap(shuffle_row)(jax.random.split(keys[5], SET_TOK), chosen_ids)


def draw_expert_ids(key, part):
    keys = jax.random.split(jax.random.fold_in(key, 17), SETS)
    return jax.vmap(draw_one_set)(keys).astype(jnp.int32)


def with_ends(array, key, low, high):
    index_at = [jax.random.randint(jax.random.fold_in(key, axis), (), 0, length) for axis, length in enumerate(array.shape)]
    longest = array.shape.index(max(array.shape))
    beside = index_at[:longest] + [(index_at[longest] + 1) % array.shape[longest]] + index_at[longest + 1:]
    return array.at[tuple(index_at)].set(low).at[tuple(beside)].set(high)


def block_levels(key, shape, pieces, smallest, largest):
    def one(axis_at, blocks):
        steps = jax.random.uniform(jax.random.fold_in(jax.random.fold_in(key, 6), axis_at), (blocks,), jnp.float32, smallest / len(pieces), largest / len(pieces))
        return jnp.repeat(jnp.exp(steps), shape[axis_at] // blocks).reshape((-1,) + (1,) * (len(shape) - axis_at - 1))

    level = one(*pieces[0])
    for cut in pieces[1:]:
        level = level * one(*cut)
    return level


def noise(rng, dims, deviation, bound, shards=(), kind=jnp.bfloat16):
    array = deviation * jax.random.normal(rng, dims, jnp.float32)
    if shards:
        array = array * block_levels(rng, dims, shards, -0.22, 0.18)
    return jnp.clip(array, -bound, bound).astype(kind)


def setup_inputs(seed: int = 0) -> dict:
    key_of = jax.random.split(jax.random.key(seed), 7)
    return {
        "tokens": noise(key_of[0], (SETS, SET_TOK, D), 1.0, 6.0, ((0, 64), (1, 16))),
        "expert_ids": draw_expert_ids(jax.random.fold_in(key_of[6], 71), 0),
        "gate_codes": with_ends(jax.random.randint(key_of[2], (SETS, SET_TOK, TOP), 1, 1024), jax.random.fold_in(key_of[2], 1), 1, 1023).astype(jnp.int32),
        "w_gate": noise(key_of[3], (EXPERTS, D, FF), D ** -0.5, 0.0625, ((0, 32), (2, 16))),
        "w_up": noise(key_of[4], (EXPERTS, D, FF), D ** -0.5, 0.0625, ((0, 32), (2, 16))),
        "w_down": noise(key_of[5], (EXPERTS, FF, D), FF ** -0.5, 0.125, ((0, 32), (1, 16))),
    }


def routing(expert_ids, gate_codes):
    codes = gate_codes.astype(jnp.float32)
    gates = 2.5 * codes / jnp.sum(codes, axis=-1, keepdims=True)
    window = jnp.arange(EXPERTS, dtype=jnp.int32)
    hits = expert_ids[..., None] == window
    member = jnp.any(hits, axis=-2).astype(jnp.int32)
    weight = jnp.sum(jnp.where(hits, gates[..., None], jnp.float32(0.0)), axis=-2)
    rank = jnp.cumsum(member, axis=-2) - member
    slots = jnp.arange(CAPG, dtype=jnp.int32)
    place = (member[..., None] == 1) & (rank[..., None] == slots)
    return place, weight


def reference(tokens, expert_ids, gate_codes, w_gate, w_up, w_down):
    place, weight = routing(expert_ids, gate_codes)
    pick = place.astype(jnp.float32)
    rows = jnp.einsum("stej,std->sejd", pick, tokens.astype(jnp.float32)).astype(jnp.bfloat16)
    slices = N_GROUP
    hid_dev = FF // slices

    def one_expert(items):
        expert_rows, gate_mat, up_mat, down_mat = items
        flat = expert_rows.reshape(SETS * CAPG, D)
        first = jnp.dot(flat, gate_mat, preferred_element_type=jnp.float32)
        second = jnp.dot(flat, up_mat, preferred_element_type=jnp.float32)
        hidden = (jax.nn.silu(first) * second).astype(jnp.bfloat16)
        parts = jnp.einsum("rgh,ghd->grd", hidden.reshape(SETS * CAPG, slices, hid_dev).astype(jnp.float32),
                           down_mat.reshape(slices, hid_dev, D).astype(jnp.float32))
        parts = lax.optimization_barrier(parts.astype(jnp.bfloat16)).astype(jnp.float32)
        return jnp.sum(parts, axis=0).reshape(SETS, CAPG, D)

    outs = lax.map(one_expert, (jnp.transpose(rows, (1, 0, 2, 3)), w_gate, w_up, w_down))
    mix = jnp.where(place, weight[..., None], jnp.float32(0.0))
    mixed = jnp.einsum("stej,esjd->std", mix, outs, precision=lax.Precision.HIGHEST)
    return mixed.astype(jnp.bfloat16)
```

```python
import jax
import jax.numpy as jnp
from jax import lax
from jax.sharding import Mesh
from jax.sharding import PartitionSpec as P


CAPG = 4
GROUP = ("y", "xh")
EXPERT = ("z", "core")
SETS_OVER = ("z", "core", "dp")


def exchange(parts, axes):
    return lax.all_to_all(parts, axes, 0, 0, tiled=True)


def in_columns(rows, pieces):
    cols = rows.shape[1] // pieces
    return jnp.stack([rows[:, i * cols : (i + 1) * cols] for i in range(pieces)])


def routing(expert_ids, gate_codes, experts, capacity):
    window = jnp.arange(experts, dtype=jnp.int32)
    hits = expert_ids[..., None] == window
    member = jnp.any(hits, axis=-2)
    codes = gate_codes.astype(jnp.float32)
    gates = 2.5 * codes / jnp.sum(codes, axis=-1, keepdims=True)
    weight = jnp.sum(jnp.where(hits, gates[..., None], jnp.float32(0.0)), axis=-2)
    tokens = expert_ids.shape[0]
    before = jnp.tril(jnp.ones((tokens, tokens), jnp.bfloat16), -1)
    rank = jnp.dot(before, member.astype(jnp.bfloat16), preferred_element_type=jnp.float32)
    slots = jnp.arange(capacity, dtype=jnp.float32)
    place = member[..., None] & (rank[..., None] == slots)
    return place, weight


def around(shard, axis):
    n = lax.axis_size(axis)
    up = [(i, (i + 1) % n) for i in range(n)]
    down = [(i, (i - 1) % n) for i in range(n)]
    found = [(0, shard)]
    a = b = shard
    for k in range(1, n // 2 + 1):
        a = lax.ppermute(a, axis, up)
        found.append((-k, a))
        if 2 * k < n:
            b = lax.ppermute(b, axis, down)
            found.append((k, b))
    return found


def per_device(tokens, expert_ids, gate_codes, w_gate, w_up, w_down):
    ny, nh = lax.axis_size("y"), lax.axis_size("xh")
    experts = lax.axis_size(EXPERT)
    own, width = tokens.shape[1], tokens.shape[2]
    cols = width // ny
    hid = w_gate.shape[2]
    here = lax.axis_index("y")

    blocks = in_columns(tokens[0], ny)
    blocks = jnp.broadcast_to(blocks[:, None], (ny, nh, own, cols))
    toks = exchange(blocks.reshape(ny * nh, own, cols), GROUP)
    blocks = [w_down[0][:, i * cols : (i + 1) * cols] for i in range(ny)]
    blocks = jnp.stack(blocks)
    downs = {}
    for k in sorted(range(1, ny), key=lambda k: -min(k, ny - k)):
        block = lax.dynamic_index_in_dim(blocks, lax.rem(here + k, ny), 0, keepdims=False)
        downs[k] = lax.ppermute(block, "y", [(i, (i + k) % ny) for i in range(ny)])
    downs[0] = lax.dynamic_index_in_dim(blocks, here, 0, keepdims=False)

    place, weight = routing(expert_ids[0], gate_codes[0], experts, CAPG)
    mix = jnp.where(place, weight[..., None], jnp.float32(0.0))
    rows = jnp.einsum(
        "tej,td->ejd",
        place.astype(jnp.bfloat16),
        toks.reshape(ny * nh * own, cols),
        preferred_element_type=jnp.float32,
    ).astype(jnp.bfloat16)
    got = exchange(rows, EXPERT)
    sets = got.shape[0]
    count = sets * CAPG
    gate_blocks = w_gate[0].reshape(ny, cols, hid)
    up_blocks = w_up[0].reshape(ny, cols, hid)
    first = second = jnp.float32(0.0)
    for step, shard in around(got.reshape(count, cols), "y"):
        at = lax.rem(here + step + ny, ny)
        gate = lax.dynamic_index_in_dim(gate_blocks, at, 0, keepdims=False)
        up = lax.dynamic_index_in_dim(up_blocks, at, 0, keepdims=False)
        first += jnp.dot(shard, gate, preferred_element_type=jnp.float32)
        second += jnp.dot(shard, up, preferred_element_type=jnp.float32)
    hidden = (jax.nn.silu(first) * second).astype(jnp.bfloat16)
    hiddens = exchange(jnp.broadcast_to(hidden[None], (ny, count, hid)), "y")
    outs = jnp.float32(0.0)
    for k in range(ny):
        part = lax.dynamic_index_in_dim(hiddens, lax.rem(here - k + ny, ny), 0, keepdims=False)
        outs += jnp.dot(part, downs[k], preferred_element_type=jnp.float32)
    outs = outs.astype(jnp.bfloat16)
    back = exchange(outs.reshape(sets, CAPG, cols), EXPERT)
    mixed = jnp.einsum(
        "tej,ejc->tc",
        mix,
        back.astype(jnp.float32),
        precision=lax.Precision.HIGHEST,
        preferred_element_type=jnp.float32,
    )
    home = exchange(mixed.astype(jnp.bfloat16).reshape(ny * nh, own, cols), GROUP)
    home = home.reshape(ny, nh, own, cols).astype(jnp.float32)
    home = jnp.sum(home, axis=1).astype(jnp.bfloat16)
    return jnp.concatenate([home[i] for i in range(ny)], axis=1)[None]


def solution(mesh):
    fine = Mesh(
        mesh.devices.reshape(8, 2, 16, 2, mesh.shape["dp"]), ("y", "xh", "z", "core", "dp")
    )
    placed = (
        P(SETS_OVER, GROUP, None),
        P(SETS_OVER, None, None),
        P(SETS_OVER, None, None),
        P(EXPERT, None, GROUP),
        P(EXPERT, None, GROUP),
        P(EXPERT, GROUP, None),
    )
    return jax.shard_map(
        per_device,
        mesh=fine,
        in_specs=placed,
        out_specs=P(SETS_OVER, GROUP, None),
        check_vma=False,
    )
```

```python
import jax
import jax.numpy as jnp
from jax import lax
from jax.experimental import pallas as pl
from jax.experimental.pallas import tpu as pltpu
from jax.sharding import Mesh
from jax.sharding import PartitionSpec as P


CAPG = 4
GROUP = ("y", "xh")
EXPERT = ("z", "core")
SETS_OVER = ("z", "core", "dp")


def exchange(parts, axes):
    return lax.all_to_all(parts, axes, 0, 0, tiled=True)


def vmem():
    return pl.BlockSpec(memory_space=pltpu.VMEM)


def in_vmem(x):
    return pltpu.with_memory_space_constraint(x, pltpu.VMEM)


def anywhere():
    return pl.BlockSpec(memory_space=pl.ANY)


def in_columns(rows, pieces, copies):
    own, width = rows.shape
    cols = width // pieces

    def kernel(rows_ref, out_ref):
        for i in range(pieces):
            piece = rows_ref[:, i * cols : (i + 1) * cols]
            for j in range(copies):
                out_ref[i * copies + j] = piece

    return pl.pallas_call(
        kernel,
        out_shape=jax.ShapeDtypeStruct((pieces * copies, own, cols), rows.dtype),
        in_specs=[vmem()],
        out_specs=vmem(),
        name="in_columns",
    )(rows)


def cut_ahead(matrix, axis):
    n = lax.axis_size(axis)
    rows, width = matrix.shape
    cols = width // n

    def kernel(matrix_ref, *refs):
        outs, sems = refs[:n], refs[n]
        here = lax.axis_index(axis)
        copies = []
        for k in range(n):
            at = pl.multiple_of(lax.rem(here + k, n) * cols, cols)
            copies.append(
                pltpu.make_async_copy(matrix_ref.at[:, pl.ds(at, cols)], outs[k], sems.at[k])
            )
        for copy in copies:
            copy.start()
        for copy in copies:
            copy.wait()

    return pl.pallas_call(
        kernel,
        out_shape=[jax.ShapeDtypeStruct((rows, cols), matrix.dtype)] * n,
        in_specs=[anywhere()],
        out_specs=[anywhere()] * n,
        scratch_shapes=[pltpu.SemaphoreType.DMA((n,))],
        name="cut_ahead",
    )(matrix)


def down_product(hiddens, downs, axis):
    n = lax.axis_size(axis)
    rows = hiddens.shape[1]
    cols = downs[0].shape[1]

    def kernel(hid_ref, *refs):
        outs_ref = refs[n]
        here = lax.axis_index(axis)
        total = jnp.zeros((rows, cols), jnp.float32)
        for k in range(n):
            part = hid_ref[lax.rem(here - k + n, n)]
            total += jnp.dot(part, refs[k][...], preferred_element_type=jnp.float32)
        outs_ref[...] = total.astype(outs_ref.dtype)

    return pl.pallas_call(
        kernel,
        out_shape=jax.ShapeDtypeStruct((rows, cols), jnp.bfloat16),
        in_specs=[vmem()] * (n + 1),
        out_specs=vmem(),
        name="down_product",
    )(*(in_vmem(x) for x in (hiddens, *downs)))


def routing(expert_ids, gate_codes, experts, capacity):
    window = jnp.arange(experts, dtype=jnp.int32)
    hits = expert_ids[..., None] == window
    member = jnp.any(hits, axis=-2)
    codes = gate_codes.astype(jnp.float32)
    gates = 2.5 * codes / jnp.sum(codes, axis=-1, keepdims=True)
    weight = jnp.sum(jnp.where(hits, gates[..., None], jnp.float32(0.0)), axis=-2)
    tokens = expert_ids.shape[0]
    before = jnp.tril(jnp.ones((tokens, tokens), jnp.bfloat16), -1)
    rank = jnp.dot(before, member.astype(jnp.bfloat16), preferred_element_type=jnp.float32)
    slots = jnp.arange(capacity, dtype=jnp.float32)
    place = member[..., None] & (rank[..., None] == slots)
    return place, weight


def around(shard, axis):
    n = lax.axis_size(axis)
    up = [(i, (i + 1) % n) for i in range(n)]
    down = [(i, (i - 1) % n) for i in range(n)]
    found = [(0, shard)]
    a = b = shard
    for k in range(1, n // 2 + 1):
        a = lax.ppermute(a, axis, up)
        found.append((-k, a))
        if 2 * k < n:
            b = lax.ppermute(b, axis, down)
            found.append((k, b))
    return found


def per_device(tokens, expert_ids, gate_codes, w_gate, w_up, w_down):
    ny, nh = lax.axis_size("y"), lax.axis_size("xh")
    experts = lax.axis_size(EXPERT)
    own, width = tokens.shape[1], tokens.shape[2]
    cols = width // ny
    hid = w_gate.shape[2]
    here = lax.axis_index("y")

    toks = exchange(in_columns(tokens[0], ny, nh), GROUP)
    downs = list(cut_ahead(w_down[0], "y"))
    for k in range(1, ny):
        downs[k] = lax.ppermute(downs[k], "y", [(i, (i + k) % ny) for i in range(ny)])

    place, weight = routing(expert_ids[0], gate_codes[0], experts, CAPG)
    mix = jnp.where(place, weight[..., None], jnp.float32(0.0))
    rows = jnp.einsum(
        "tej,td->ejd",
        place.astype(jnp.bfloat16),
        toks.reshape(ny * nh * own, cols),
        preferred_element_type=jnp.float32,
    ).astype(jnp.bfloat16)
    got = exchange(rows, EXPERT)
    sets = got.shape[0]
    count = sets * CAPG
    gate_blocks = w_gate[0].reshape(ny, cols, hid)
    up_blocks = w_up[0].reshape(ny, cols, hid)
    first = second = jnp.float32(0.0)
    for step, shard in around(got.reshape(count, cols), "y"):
        at = lax.rem(here + step + ny, ny)
        gate = lax.dynamic_index_in_dim(gate_blocks, at, 0, keepdims=False)
        up = lax.dynamic_index_in_dim(up_blocks, at, 0, keepdims=False)
        first += jnp.dot(shard, gate, preferred_element_type=jnp.float32)
        second += jnp.dot(shard, up, preferred_element_type=jnp.float32)
    hidden = (jax.nn.silu(first) * second).astype(jnp.bfloat16)
    hiddens = exchange(jnp.broadcast_to(hidden[None], (ny, count, hid)), "y")
    outs = down_product(hiddens, downs, "y")
    back = exchange(outs.reshape(sets, CAPG, cols), EXPERT)
    mixed = jnp.einsum(
        "tej,ejc->tc",
        mix,
        back.astype(jnp.float32),
        precision=lax.Precision.HIGHEST,
        preferred_element_type=jnp.float32,
    )
    home = exchange(mixed.astype(jnp.bfloat16).reshape(ny * nh, own, cols), GROUP)
    home = home.reshape(ny, nh, own, cols).astype(jnp.float32)
    home = jnp.sum(home, axis=1).astype(jnp.bfloat16)
    return jnp.concatenate([home[i] for i in range(ny)], axis=1)[None]


def solution(mesh):
    fine = Mesh(
        mesh.devices.reshape(8, 2, 16, 2, mesh.shape["dp"]), ("y", "xh", "z", "core", "dp")
    )
    placed = (
        P(SETS_OVER, GROUP, None),
        P(SETS_OVER, None, None),
        P(SETS_OVER, None, None),
        P(EXPERT, None, GROUP),
        P(EXPERT, None, GROUP),
        P(EXPERT, GROUP, None),
    )
    return jax.shard_map(
        per_device,
        mesh=fine,
        in_specs=placed,
        out_specs=P(SETS_OVER, GROUP, None),
        check_vma=False,
    )
```

```python
import jax
import jax.numpy as jnp
from jax import lax
from jax.experimental import pallas as pl
from jax.experimental.pallas import tpu as pltpu
from jax.sharding import Mesh
from jax.sharding import PartitionSpec as P


CAPG = 4
GROUP = ("y", "xh")
EXPERT = ("z", "core")
SETS_OVER = ("z", "core", "dp")


def exchange(parts, axes):
    return lax.all_to_all(parts, axes, 0, 0, tiled=True)


SMALL = pltpu.CompilerParams(vmem_limit_bytes=8 * 2**20)


def vmem():
    return pl.BlockSpec(memory_space=pltpu.VMEM)


def in_vmem(x):
    return pltpu.with_memory_space_constraint(x, pltpu.VMEM)


def anywhere():
    return pl.BlockSpec(memory_space=pl.ANY)


def in_columns(rows, pieces, copies):
    own, width = rows.shape
    cols = width // pieces

    def kernel(rows_ref, out_ref):
        for i in range(pieces):
            piece = rows_ref[:, i * cols : (i + 1) * cols]
            for j in range(copies):
                out_ref[i * copies + j] = piece

    return pl.pallas_call(
        kernel,
        out_shape=jax.ShapeDtypeStruct((pieces * copies, own, cols), rows.dtype),
        in_specs=[vmem()],
        out_specs=vmem(),
        name="in_columns",
        compiler_params=SMALL,
    )(rows)


def cut_ahead(matrix, axis):
    n = lax.axis_size(axis)
    rows, width = matrix.shape
    cols = width // n

    def kernel(matrix_ref, *refs):
        outs, sems = refs[:n], refs[n]
        here = lax.axis_index(axis)
        copies = []
        for k in range(n):
            at = pl.multiple_of(lax.rem(here + k, n) * cols, cols)
            copies.append(
                pltpu.make_async_copy(matrix_ref.at[:, pl.ds(at, cols)], outs[k], sems.at[k])
            )
        for copy in copies:
            copy.start()
        for copy in copies:
            copy.wait()

    return pl.pallas_call(
        kernel,
        out_shape=[pltpu.VMEM((rows, cols), matrix.dtype)] * n,
        in_specs=[anywhere()],
        out_specs=[vmem()] * n,
        scratch_shapes=[pltpu.SemaphoreType.DMA((n,))],
        name="cut_ahead",
        compiler_params=SMALL,
    )(pltpu.with_memory_space_constraint(matrix, pltpu.HBM))


def gate_up_step(sums, shard, gate, up, step, axis):
    n = lax.axis_size(axis)
    rows, cols = shard.shape
    hid = gate.shape[1]
    first = sums is None

    def kernel(*refs):
        shard_ref, gate_ref, up_ref = refs[:3]
        here = lax.axis_index(axis)
        at = pl.multiple_of(lax.rem(here + step + n, n) * cols, cols)
        block = shard_ref[...]
        for i, weight in enumerate((gate_ref, up_ref)):
            got = jnp.dot(block, weight[pl.ds(at, cols), :], preferred_element_type=jnp.float32)
            refs[-2 + i][...] = got if first else refs[3 + i][...] + got

    return pl.pallas_call(
        kernel,
        out_shape=[pltpu.VMEM((rows, hid), jnp.float32)] * 2,
        in_specs=[vmem()] * (3 if first else 5),
        out_specs=[vmem()] * 2,
        name="gate_up_step",
        compiler_params=SMALL,
    )(*(in_vmem(x) for x in (shard, gate, up, *(sums or ()))))


def down_product(hiddens, downs, axis):
    n = lax.axis_size(axis)
    rows = hiddens.shape[1]
    cols = downs[0].shape[1]

    def kernel(hid_ref, *refs):
        outs_ref = refs[n]
        here = lax.axis_index(axis)
        total = jnp.zeros((rows, cols), jnp.float32)
        for k in range(n):
            part = hid_ref[lax.rem(here - k + n, n)]
            total += jnp.dot(part, refs[k][...], preferred_element_type=jnp.float32)
        outs_ref[...] = total.astype(outs_ref.dtype)

    return pl.pallas_call(
        kernel,
        out_shape=jax.ShapeDtypeStruct((rows, cols), jnp.bfloat16),
        in_specs=[vmem()] * (n + 1),
        out_specs=vmem(),
        name="down_product",
        compiler_params=SMALL,
    )(*(in_vmem(x) for x in (hiddens, *downs)))


def routing(expert_ids, gate_codes, experts, capacity):
    window = jnp.arange(experts, dtype=jnp.int32)
    hits = expert_ids[..., None] == window
    member = jnp.any(hits, axis=-2)
    codes = gate_codes.astype(jnp.float32)
    gates = 2.5 * codes / jnp.sum(codes, axis=-1, keepdims=True)
    weight = jnp.sum(jnp.where(hits, gates[..., None], jnp.float32(0.0)), axis=-2)
    tokens = expert_ids.shape[0]
    before = jnp.tril(jnp.ones((tokens, tokens), jnp.bfloat16), -1)
    rank = jnp.dot(before, member.astype(jnp.bfloat16), preferred_element_type=jnp.float32)
    slots = jnp.arange(capacity, dtype=jnp.float32)
    place = member[..., None] & (rank[..., None] == slots)
    return place, weight


def around(shard, axis):
    n = lax.axis_size(axis)
    up = [(i, (i + 1) % n) for i in range(n)]
    down = [(i, (i - 1) % n) for i in range(n)]
    found = [(0, shard)]
    a = b = shard
    for k in range(1, n // 2 + 1):
        a = lax.ppermute(a, axis, up)
        found.append((-k, a))
        if 2 * k < n:
            b = lax.ppermute(b, axis, down)
            found.append((k, b))
    return found


def per_device(tokens, expert_ids, gate_codes, w_gate, w_up, w_down):
    ny, nh = lax.axis_size("y"), lax.axis_size("xh")
    experts = lax.axis_size(EXPERT)
    own, width = tokens.shape[1], tokens.shape[2]
    cols = width // ny
    hid = w_gate.shape[2]

    toks = exchange(in_columns(tokens[0], ny, nh), GROUP)
    downs = list(cut_ahead(w_down[0], "y"))
    for k in range(1, ny):
        downs[k] = lax.ppermute(downs[k], "y", [(i, (i + k) % ny) for i in range(ny)])

    place, weight = routing(expert_ids[0], gate_codes[0], experts, CAPG)
    mix = jnp.where(place, weight[..., None], jnp.float32(0.0))
    rows = jnp.einsum(
        "tej,td->ejd",
        place.astype(jnp.bfloat16),
        toks.reshape(ny * nh * own, cols),
        preferred_element_type=jnp.float32,
    ).astype(jnp.bfloat16)
    got = exchange(rows, EXPERT)
    sets = got.shape[0]
    count = sets * CAPG
    sums = None
    for step, shard in around(got.reshape(count, cols), "y"):
        sums = gate_up_step(sums, shard, w_gate[0], w_up[0], step, "y")
    first, second = sums
    hidden = (jax.nn.silu(first) * second).astype(jnp.bfloat16)
    hiddens = exchange(jnp.broadcast_to(hidden[None], (ny, count, hid)), "y")
    outs = down_product(hiddens, downs, "y")
    back = exchange(outs.reshape(sets, CAPG, cols), EXPERT)
    mixed = jnp.einsum(
        "tej,ejc->tc",
        mix,
        back.astype(jnp.float32),
        precision=lax.Precision.HIGHEST,
        preferred_element_type=jnp.float32,
    )
    home = exchange(mixed.astype(jnp.bfloat16).reshape(ny * nh, own, cols), GROUP)
    home = home.reshape(ny, nh, own, cols).astype(jnp.float32)
    home = jnp.sum(home, axis=1).astype(jnp.bfloat16)
    return jnp.concatenate([home[i] for i in range(ny)], axis=1)[None]


def solution(mesh):
    fine = Mesh(
        mesh.devices.reshape(8, 2, 16, 2, mesh.shape["dp"]), ("y", "xh", "z", "core", "dp")
    )
    placed = (
        P(SETS_OVER, GROUP, None),
        P(SETS_OVER, None, None),
        P(SETS_OVER, None, None),
        P(EXPERT, None, GROUP),
        P(EXPERT, None, GROUP),
        P(EXPERT, GROUP, None),
    )
    return jax.shard_map(
        per_device,
        mesh=fine,
        in_specs=placed,
        out_specs=P(SETS_OVER, GROUP, None),
        check_vma=False,
    )
```

```python
import jax
import jax.numpy as jnp
from jax import lax
from jax.experimental import pallas as pl
from jax.experimental.pallas import tpu as pltpu
from jax.sharding import Mesh
from jax.sharding import PartitionSpec as P


CAPG = 4
GROUP = ("y", "xh")
EXPERT = ("z", "core")
SETS_OVER = ("z", "core", "dp")


def exchange(parts, axes):
    return lax.all_to_all(parts, axes, 0, 0, tiled=True)


SMALL = pltpu.CompilerParams(vmem_limit_bytes=8 * 2**20)


def vmem():
    return pl.BlockSpec(memory_space=pltpu.VMEM)


def in_vmem(x):
    return pltpu.with_memory_space_constraint(x, pltpu.VMEM)


def anywhere():
    return pl.BlockSpec(memory_space=pl.ANY)


def in_columns(rows, pieces, copies):
    own, width = rows.shape
    cols = width // pieces

    def kernel(rows_ref, out_ref):
        for i in range(pieces):
            piece = rows_ref[:, i * cols : (i + 1) * cols]
            for j in range(copies):
                out_ref[i * copies + j] = piece

    return pl.pallas_call(
        kernel,
        out_shape=jax.ShapeDtypeStruct((pieces * copies, own, cols), rows.dtype),
        in_specs=[vmem()],
        out_specs=vmem(),
        name="in_columns",
        compiler_params=SMALL,
    )(rows)


def signed(k):
    here, side = lax.axis_index("y"), lax.axis_index("dp")
    away = 1 - 2 * side if k < 3 else 2 * side - 1
    return here, side, away * k


def cut_blocks(matrix):
    n, far = lax.axis_size("y"), lax.axis_size("y") // 2
    rows, width = matrix.shape
    cols, half = width // n, rows // 2

    def kernel(matrix_ref, *refs):
        outs, sems = refs[: far + 1], refs[far + 1]
        copies = []
        for k in range(far + 1):
            here, side, step = signed(k)
            step = far if k == far else step
            at = pl.multiple_of(lax.rem(here + step + n, n) * cols, cols)
            lines = pl.ds(pl.multiple_of(side * half, half), half) if k == far else slice(None)
            source = matrix_ref.at[lines, pl.ds(at, cols)]
            copies.append(pltpu.make_async_copy(source, outs[k], sems.at[k]))
        for copy in copies:
            copy.start()
        for copy in copies:
            copy.wait()

    whole, part = pltpu.VMEM((rows, cols), matrix.dtype), pltpu.VMEM((half, cols), matrix.dtype)
    return pl.pallas_call(
        kernel,
        out_shape=[whole] * far + [part],
        in_specs=[anywhere()],
        out_specs=[vmem()] * (far + 1),
        scratch_shapes=[pltpu.SemaphoreType.DMA((far + 1,))],
        name="cut_blocks",
        compiler_params=SMALL,
    )(pltpu.with_memory_space_constraint(matrix, pltpu.HBM))


def stacked(parts):
    counts = [p.shape[0] for p in parts]

    def kernel(*refs):
        at = 0
        for ref, count in zip(refs, counts):
            refs[-1][at : at + count, :] = ref[...]
            at += count

    return pl.pallas_call(
        kernel,
        out_shape=pltpu.VMEM((sum(counts), parts[0].shape[1]), parts[0].dtype),
        in_specs=[vmem()] * len(parts),
        out_specs=vmem(),
        name="stacked",
        compiler_params=SMALL,
    )(*parts)


def down_product(hiddens, own, mine, others):
    n, far = lax.axis_size("y"), lax.axis_size("y") // 2
    rows, hid = hiddens.shape[1:]
    half, cols = hid // 2, own.shape[1]

    def kernel(hid_ref, own_ref, mine_ref, others_ref, outs_ref, far_ref):
        here, side, _ = signed(1)
        total = jnp.dot(hid_ref[here], own_ref[...], preferred_element_type=jnp.float32)
        for k in range(1, far):
            _, _, step = signed(k)
            lines = slice((k - 1) * hid, k * hid)
            for sign, ref in ((1, mine_ref), (-1, others_ref)):
                part = hid_ref[lax.rem(here - sign * step + n, n)]
                total += jnp.dot(part, ref[lines, :], preferred_element_type=jnp.float32)
        lines = slice((far - 1) * hid, (far - 1) * hid + half)
        far_ref[pl.ds(pl.multiple_of(side * half, half), half), :] = mine_ref[lines, :]
        far_ref[pl.ds(pl.multiple_of((1 - side) * half, half), half), :] = others_ref[lines, :]
        part = hid_ref[lax.rem(here + far, n)]
        total += jnp.dot(part, far_ref[...], preferred_element_type=jnp.float32)
        outs_ref[...] = total.astype(outs_ref.dtype)

    return pl.pallas_call(
        kernel,
        out_shape=jax.ShapeDtypeStruct((rows, cols), jnp.bfloat16),
        in_specs=[vmem()] * 4,
        out_specs=vmem(),
        scratch_shapes=[pltpu.VMEM((hid, cols), own.dtype)],
        name="down_product",
        compiler_params=SMALL,
    )(*(in_vmem(x) for x in (hiddens, own, mine, others)))


def gate_up_step(sums, shard, gate, up, step, axis):
    n = lax.axis_size(axis)
    rows, cols = shard.shape
    hid = gate.shape[1]
    first = sums is None

    def kernel(*refs):
        shard_ref, gate_ref, up_ref = refs[:3]
        here = lax.axis_index(axis)
        at = pl.multiple_of(lax.rem(here + step + n, n) * cols, cols)
        block = shard_ref[...]
        for i, weight in enumerate((gate_ref, up_ref)):
            got = jnp.dot(block, weight[pl.ds(at, cols), :], preferred_element_type=jnp.float32)
            refs[-2 + i][...] = got if first else refs[3 + i][...] + got

    return pl.pallas_call(
        kernel,
        out_shape=[pltpu.VMEM((rows, hid), jnp.float32)] * 2,
        in_specs=[vmem()] * (3 if first else 5),
        out_specs=[vmem()] * 2,
        name="gate_up_step",
        compiler_params=SMALL,
    )(*(in_vmem(x) for x in (shard, gate, up, *(sums or ()))))


def routing(expert_ids, gate_codes, experts, capacity):
    window = jnp.arange(experts, dtype=jnp.int32)
    hits = expert_ids[..., None] == window
    member = jnp.any(hits, axis=-2)
    codes = gate_codes.astype(jnp.float32)
    gates = 2.5 * codes / jnp.sum(codes, axis=-1, keepdims=True)
    weight = jnp.sum(jnp.where(hits, gates[..., None], jnp.float32(0.0)), axis=-2)
    tokens = expert_ids.shape[0]
    before = jnp.tril(jnp.ones((tokens, tokens), jnp.bfloat16), -1)
    rank = jnp.dot(before, member.astype(jnp.bfloat16), preferred_element_type=jnp.float32)
    slots = jnp.arange(capacity, dtype=jnp.float32)
    place = member[..., None] & (rank[..., None] == slots)
    return place, weight


def around(shard, axis):
    n = lax.axis_size(axis)
    up = [(i, (i + 1) % n) for i in range(n)]
    down = [(i, (i - 1) % n) for i in range(n)]
    found = [(0, shard)]
    a = b = shard
    for k in range(1, n // 2 + 1):
        a = lax.ppermute(a, axis, up)
        found.append((-k, a))
        if 2 * k < n:
            b = lax.ppermute(b, axis, down)
            found.append((k, b))
    return found


def per_device(tokens, expert_ids, gate_codes, w_gate, w_up, w_down):
    ny, nh = lax.axis_size("y"), lax.axis_size("xh")
    experts = lax.axis_size(EXPERT)
    own, width = tokens.shape[1], tokens.shape[2]
    cols = width // ny
    hid = w_gate.shape[2]

    toks = exchange(in_columns(tokens[0], ny, nh), GROUP)
    own_block, *blocks = cut_blocks(w_down[0])
    sides = lax.axis_size("dp")
    for k in range(1, ny // 2 + 1):
        pairs = []
        for i in range(ny):
            for side in range(sides):
                away = k if (side == 0) == (k != 3) else -k
                pairs.append((i * sides + side, (i + away) % ny * sides + side))
        blocks[k - 1] = lax.ppermute(blocks[k - 1], ("y", "dp"), pairs)
    mine = stacked(blocks)
    others = lax.ppermute(mine, "dp", [(0, 1), (1, 0)])

    place, weight = routing(expert_ids[0], gate_codes[0], experts, CAPG)
    mix = jnp.where(place, weight[..., None], jnp.float32(0.0))
    rows = jnp.einsum(
        "tej,td->ejd",
        place.astype(jnp.bfloat16),
        toks.reshape(ny * nh * own, cols),
        preferred_element_type=jnp.float32,
    ).astype(jnp.bfloat16)
    got = exchange(rows, EXPERT)
    sets = got.shape[0]
    count = sets * CAPG
    sums = None
    for step, shard in around(got.reshape(count, cols), "y"):
        sums = gate_up_step(sums, shard, w_gate[0], w_up[0], step, "y")
    first, second = sums
    hidden = (jax.nn.silu(first) * second).astype(jnp.bfloat16)
    hiddens = exchange(jnp.broadcast_to(hidden[None], (ny, count, hid)), "y")
    outs = down_product(hiddens, own_block, mine, others)
    back = exchange(outs.reshape(sets, CAPG, cols), EXPERT)
    mixed = jnp.einsum(
        "tej,ejc->tc",
        mix,
        back.astype(jnp.float32),
        precision=lax.Precision.HIGHEST,
        preferred_element_type=jnp.float32,
    )
    home = exchange(mixed.astype(jnp.bfloat16).reshape(ny * nh, own, cols), GROUP)
    home = home.reshape(ny, nh, own, cols).astype(jnp.float32)
    home = jnp.sum(home, axis=1).astype(jnp.bfloat16)
    return jnp.concatenate([home[i] for i in range(ny)], axis=1)[None]


def solution(mesh):
    fine = Mesh(
        mesh.devices.reshape(8, 2, 16, 2, mesh.shape["dp"]), ("y", "xh", "z", "core", "dp")
    )
    placed = (
        P(SETS_OVER, GROUP, None),
        P(SETS_OVER, None, None),
        P(SETS_OVER, None, None),
        P(EXPERT, None, GROUP),
        P(EXPERT, None, GROUP),
        P(EXPERT, GROUP, None),
    )
    return jax.shard_map(
        per_device,
        mesh=fine,
        in_specs=placed,
        out_specs=P(SETS_OVER, GROUP, None),
        check_vma=False,
    )
```

```python
import jax
import jax.numpy as jnp
from jax import lax
from jax.experimental import pallas as pl
from jax.experimental.pallas import tpu as pltpu
from jax.sharding import Mesh
from jax.sharding import PartitionSpec as P


CAPG = 4
GROUP = ("y", "xh")
EXPERT = ("z", "core")
SETS_OVER = ("z", "core", "dp")


def exchange(parts, axes):
    return lax.all_to_all(parts, axes, 0, 0, tiled=True)


SMALL = pltpu.CompilerParams(vmem_limit_bytes=8 * 2**20)


def vmem():
    return pl.BlockSpec(memory_space=pltpu.VMEM)


def in_vmem(x):
    return pltpu.with_memory_space_constraint(x, pltpu.VMEM)


def anywhere():
    return pl.BlockSpec(memory_space=pl.ANY)


def in_columns(rows, pieces, copies):
    own, width = rows.shape
    cols = width // pieces

    def kernel(rows_ref, out_ref):
        for i in range(pieces):
            piece = rows_ref[:, i * cols : (i + 1) * cols]
            for j in range(copies):
                out_ref[i * copies + j] = piece

    return pl.pallas_call(
        kernel,
        out_shape=jax.ShapeDtypeStruct((pieces * copies, own, cols), rows.dtype),
        in_specs=[vmem()],
        out_specs=vmem(),
        name="in_columns",
        compiler_params=SMALL,
    )(rows)


def signed(k):
    here, side = lax.axis_index("y"), lax.axis_index("dp")
    away = 1 - 2 * side if k < 3 else 2 * side - 1
    return here, side, away * k


def cut_blocks(matrix):
    n, far = lax.axis_size("y"), lax.axis_size("y") // 2
    rows, width = matrix.shape
    cols, half = width // n, rows // 2

    def kernel(matrix_ref, *refs):
        outs, sems = refs[: far + 1], refs[far + 1]
        copies = []
        for k in range(far + 1):
            here, side, step = signed(k)
            step = far if k == far else step
            at = pl.multiple_of(lax.rem(here + step + n, n) * cols, cols)
            lines = pl.ds(pl.multiple_of(side * half, half), half) if k == far else slice(None)
            source = matrix_ref.at[lines, pl.ds(at, cols)]
            copies.append(pltpu.make_async_copy(source, outs[k], sems.at[k]))
        for copy in copies:
            copy.start()
        for copy in copies:
            copy.wait()

    whole, part = pltpu.VMEM((rows, cols), matrix.dtype), pltpu.VMEM((half, cols), matrix.dtype)
    return pl.pallas_call(
        kernel,
        out_shape=[whole] * far + [part],
        in_specs=[anywhere()],
        out_specs=[vmem()] * (far + 1),
        scratch_shapes=[pltpu.SemaphoreType.DMA((far + 1,))],
        name="cut_blocks",
        compiler_params=SMALL,
    )(pltpu.with_memory_space_constraint(matrix, pltpu.HBM))


def stacked(parts):
    counts = [p.shape[0] for p in parts]
    total, cols = sum(counts), parts[0].shape[1]

    def kernel(*refs):
        out_ref, sems = refs[-2:]
        copies, at = [], 0
        for k, count in enumerate(counts):
            place = out_ref.at[pl.ds(at, count), :]
            copies.append(pltpu.make_async_copy(refs[k], place, sems.at[k]))
            at += count
        for copy in copies:
            copy.start()
        for copy in copies:
            copy.wait()

    return pl.pallas_call(
        kernel,
        out_shape=pltpu.VMEM((total, cols), parts[0].dtype),
        in_specs=[anywhere()] * len(parts),
        out_specs=vmem(),
        scratch_shapes=[pltpu.SemaphoreType.DMA((len(parts),))],
        name="stacked",
        compiler_params=SMALL,
    )(*(pltpu.with_memory_space_constraint(p, pltpu.HBM) for p in parts))


def down_product(hiddens, own, mine, others):
    n, far = lax.axis_size("y"), lax.axis_size("y") // 2
    rows, hid = hiddens.shape[1:]
    half, cols = hid // 2, own.shape[1]

    def kernel(hid_ref, own_ref, mine_ref, others_ref, outs_ref, far_ref):
        here, side, _ = signed(1)
        total = jnp.dot(hid_ref[here], own_ref[...], preferred_element_type=jnp.float32)
        for k in range(1, far):
            _, _, step = signed(k)
            lines = slice((k - 1) * hid, k * hid)
            for sign, ref in ((1, mine_ref), (-1, others_ref)):
                part = hid_ref[lax.rem(here - sign * step + n, n)]
                total += jnp.dot(part, ref[lines, :], preferred_element_type=jnp.float32)
        lines = slice((far - 1) * hid, (far - 1) * hid + half)
        far_ref[pl.ds(pl.multiple_of(side * half, half), half), :] = mine_ref[lines, :]
        far_ref[pl.ds(pl.multiple_of((1 - side) * half, half), half), :] = others_ref[lines, :]
        part = hid_ref[lax.rem(here + far, n)]
        total += jnp.dot(part, far_ref[...], preferred_element_type=jnp.float32)
        outs_ref[...] = total.astype(outs_ref.dtype)

    return pl.pallas_call(
        kernel,
        out_shape=jax.ShapeDtypeStruct((rows, cols), jnp.bfloat16),
        in_specs=[vmem()] * 4,
        out_specs=vmem(),
        scratch_shapes=[pltpu.VMEM((hid, cols), own.dtype)],
        name="down_product",
        compiler_params=SMALL,
    )(*(in_vmem(x) for x in (hiddens, own, mine, others)))


def gate_up_step(sums, shard, gate, up, step, axis):
    n = lax.axis_size(axis)
    rows, cols = shard.shape
    hid = gate.shape[1]
    first = sums is None

    def kernel(*refs):
        shard_ref, gate_ref, up_ref = refs[:3]
        here = lax.axis_index(axis)
        at = pl.multiple_of(lax.rem(here + step + n, n) * cols, cols)
        block = shard_ref[...]
        for i, weight in enumerate((gate_ref, up_ref)):
            got = jnp.dot(block, weight[pl.ds(at, cols), :], preferred_element_type=jnp.float32)
            refs[-2 + i][...] = got if first else refs[3 + i][...] + got

    return pl.pallas_call(
        kernel,
        out_shape=[pltpu.VMEM((rows, hid), jnp.float32)] * 2,
        in_specs=[vmem()] * (3 if first else 5),
        out_specs=[vmem()] * 2,
        name="gate_up_step",
        compiler_params=SMALL,
    )(*(in_vmem(x) for x in (shard, gate, up, *(sums or ()))))


def routing(expert_ids, gate_codes, experts, capacity):
    window = jnp.arange(experts, dtype=jnp.int32)
    hits = expert_ids[..., None] == window
    member = jnp.any(hits, axis=-2)
    codes = gate_codes.astype(jnp.float32)
    gates = 2.5 * codes / jnp.sum(codes, axis=-1, keepdims=True)
    weight = jnp.sum(jnp.where(hits, gates[..., None], jnp.float32(0.0)), axis=-2)
    tokens = expert_ids.shape[0]
    before = jnp.tril(jnp.ones((tokens, tokens), jnp.bfloat16), -1)
    rank = jnp.dot(before, member.astype(jnp.bfloat16), preferred_element_type=jnp.float32)
    slots = jnp.arange(capacity, dtype=jnp.float32)
    place = member[..., None] & (rank[..., None] == slots)
    return place, weight


def around(shard, axis):
    n = lax.axis_size(axis)
    up = [(i, (i + 1) % n) for i in range(n)]
    down = [(i, (i - 1) % n) for i in range(n)]
    found = [(0, shard)]
    a = b = shard
    for k in range(1, n // 2 + 1):
        a = lax.ppermute(a, axis, up)
        found.append((-k, a))
        if 2 * k < n:
            b = lax.ppermute(b, axis, down)
            found.append((k, b))
    return found


def per_device(tokens, expert_ids, gate_codes, w_gate, w_up, w_down):
    ny, nh = lax.axis_size("y"), lax.axis_size("xh")
    experts = lax.axis_size(EXPERT)
    own, width = tokens.shape[1], tokens.shape[2]
    cols = width // ny
    hid = w_gate.shape[2]

    toks = exchange(in_columns(tokens[0], ny, nh), GROUP)
    own_block, *blocks = cut_blocks(w_down[0])
    sides = lax.axis_size("dp")
    for k in range(1, ny // 2 + 1):
        pairs = []
        for i in range(ny):
            for side in range(sides):
                away = k if (side == 0) == (k != 3) else -k
                pairs.append((i * sides + side, (i + away) % ny * sides + side))
        blocks[k - 1] = lax.ppermute(blocks[k - 1], ("y", "dp"), pairs)
    mine = stacked(blocks)
    others = lax.ppermute(mine, "dp", [(0, 1), (1, 0)])

    place, weight = routing(expert_ids[0], gate_codes[0], experts, CAPG)
    mix = jnp.where(place, weight[..., None], jnp.float32(0.0))
    rows = jnp.einsum(
        "tej,td->ejd",
        place.astype(jnp.bfloat16),
        toks.reshape(ny * nh * own, cols),
        preferred_element_type=jnp.float32,
    ).astype(jnp.bfloat16)
    got = exchange(rows, EXPERT)
    sets = got.shape[0]
    count = sets * CAPG
    sums = None
    for step, shard in around(got.reshape(count, cols), "y"):
        sums = gate_up_step(sums, shard, w_gate[0], w_up[0], step, "y")
    first, second = sums
    hidden = (jax.nn.silu(first) * second).astype(jnp.bfloat16)
    hiddens = exchange(jnp.broadcast_to(hidden[None], (ny, count, hid)), "y")
    outs = down_product(hiddens, own_block, mine, others)
    back = exchange(outs.reshape(sets, CAPG, cols), EXPERT)
    mixed = jnp.einsum(
        "tej,ejc->tc",
        mix,
        back.astype(jnp.float32),
        precision=lax.Precision.HIGHEST,
        preferred_element_type=jnp.float32,
    )
    home = exchange(mixed.astype(jnp.bfloat16).reshape(ny * nh, own, cols), GROUP)
    home = home.reshape(ny, nh, own, cols).astype(jnp.float32)
    home = jnp.sum(home, axis=1).astype(jnp.bfloat16)
    return jnp.concatenate([home[i] for i in range(ny)], axis=1)[None]


def solution(mesh):
    fine = Mesh(
        mesh.devices.reshape(8, 2, 16, 2, mesh.shape["dp"]), ("y", "xh", "z", "core", "dp")
    )
    placed = (
        P(SETS_OVER, GROUP, None),
        P(SETS_OVER, None, None),
        P(SETS_OVER, None, None),
        P(EXPERT, None, GROUP),
        P(EXPERT, None, GROUP),
        P(EXPERT, GROUP, None),
    )
    return jax.shard_map(
        per_device,
        mesh=fine,
        in_specs=placed,
        out_specs=P(SETS_OVER, GROUP, None),
        check_vma=False,
    )
```

```python
import jax
import jax.numpy as jnp
from jax import lax
from jax.experimental import pallas as pl
from jax.experimental.pallas import tpu as pltpu
from jax.sharding import Mesh
from jax.sharding import PartitionSpec as P


CAPG = 4
GROUP = ("y", "xh")
EXPERT = ("z", "core")
SETS_OVER = ("z", "core", "dp")


def exchange(parts, axes):
    return lax.all_to_all(parts, axes, 0, 0, tiled=True)


SMALL = pltpu.CompilerParams(vmem_limit_bytes=8 * 2**20)


def vmem():
    return pl.BlockSpec(memory_space=pltpu.VMEM)


def in_vmem(x):
    return pltpu.with_memory_space_constraint(x, pltpu.VMEM)


def anywhere():
    return pl.BlockSpec(memory_space=pl.ANY)


def in_columns(rows, pieces, copies):
    own, width = rows.shape
    cols = width // pieces

    def kernel(rows_ref, out_ref):
        for i in range(pieces):
            piece = rows_ref[:, i * cols : (i + 1) * cols]
            for j in range(copies):
                out_ref[i * copies + j] = piece

    return pl.pallas_call(
        kernel,
        out_shape=jax.ShapeDtypeStruct((pieces * copies, own, cols), rows.dtype),
        in_specs=[vmem()],
        out_specs=vmem(),
        name="in_columns",
        compiler_params=SMALL,
    )(rows)


def signed(k):
    here, side = lax.axis_index("y"), lax.axis_index("dp")
    away = 1 - 2 * side if k < 3 else 2 * side - 1
    return here, side, away * k


def cut_blocks(matrix):
    n, far = lax.axis_size("y"), lax.axis_size("y") // 2
    rows, width = matrix.shape
    cols, half = width // n, rows // 2

    def kernel(matrix_ref, *refs):
        outs, sems = refs[: far + 1], refs[far + 1]
        copies = []
        for k in range(far + 1):
            here, side, step = signed(k)
            step = far if k == far else step
            at = pl.multiple_of(lax.rem(here + step + n, n) * cols, cols)
            lines = pl.ds(pl.multiple_of(side * half, half), half) if k == far else slice(None)
            source = matrix_ref.at[lines, pl.ds(at, cols)]
            copies.append(pltpu.make_async_copy(source, outs[k], sems.at[k]))
        for copy in copies:
            copy.start()
        for copy in copies:
            copy.wait()

    whole, part = pltpu.VMEM((rows, cols), matrix.dtype), pltpu.VMEM((half, cols), matrix.dtype)
    return pl.pallas_call(
        kernel,
        out_shape=[whole] * far + [part],
        in_specs=[anywhere()],
        out_specs=[vmem()] * (far + 1),
        scratch_shapes=[pltpu.SemaphoreType.DMA((far + 1,))],
        name="cut_blocks",
        compiler_params=SMALL,
    )(pltpu.with_memory_space_constraint(matrix, pltpu.HBM))


def stacked(parts):
    counts = [p.shape[0] for p in parts]
    total, cols = sum(counts), parts[0].shape[1]

    def kernel(*refs):
        out_ref, sems = refs[-2:]
        copies, at = [], 0
        for k, count in enumerate(counts):
            place = out_ref.at[pl.ds(at, count), :]
            copies.append(pltpu.make_async_copy(refs[k], place, sems.at[k]))
            at += count
        for copy in copies:
            copy.start()
        for copy in copies:
            copy.wait()

    return pl.pallas_call(
        kernel,
        out_shape=pltpu.VMEM((total, cols), parts[0].dtype),
        in_specs=[anywhere()] * len(parts),
        out_specs=vmem(),
        scratch_shapes=[pltpu.SemaphoreType.DMA((len(parts),))],
        name="stacked",
        compiler_params=SMALL,
    )(*(pltpu.with_memory_space_constraint(p, pltpu.HBM) for p in parts))


def down_product(hiddens, own, mine, others):
    n, far = lax.axis_size("y"), lax.axis_size("y") // 2
    rows, hid = hiddens.shape[1:]
    half, cols = hid // 2, own.shape[1]

    def kernel(hid_ref, own_ref, mine_ref, others_ref, outs_ref, far_ref):
        here, side, _ = signed(1)
        total = jnp.dot(hid_ref[here], own_ref[...], preferred_element_type=jnp.float32)
        for k in range(1, far):
            _, _, step = signed(k)
            lines = slice((k - 1) * hid, k * hid)
            for sign, ref in ((1, mine_ref), (-1, others_ref)):
                part = hid_ref[lax.rem(here - sign * step + n, n)]
                total += jnp.dot(part, ref[lines, :], preferred_element_type=jnp.float32)
        lines = slice((far - 1) * hid, (far - 1) * hid + half)
        far_ref[pl.ds(pl.multiple_of(side * half, half), half), :] = mine_ref[lines, :]
        far_ref[pl.ds(pl.multiple_of((1 - side) * half, half), half), :] = others_ref[lines, :]
        part = hid_ref[lax.rem(here + far, n)]
        total += jnp.dot(part, far_ref[...], preferred_element_type=jnp.float32)
        outs_ref[...] = total.astype(outs_ref.dtype)

    return pl.pallas_call(
        kernel,
        out_shape=jax.ShapeDtypeStruct((rows, cols), jnp.bfloat16),
        in_specs=[vmem()] * 4,
        out_specs=vmem(),
        scratch_shapes=[pltpu.VMEM((hid, cols), own.dtype)],
        name="down_product",
        compiler_params=SMALL,
    )(*(in_vmem(x) for x in (hiddens, own, mine, others)))


def gate_up_step(sums, shard, gate, up, step, axis, last):
    n = lax.axis_size(axis)
    rows, cols = shard.shape
    hid = gate.shape[1]
    first = sums is None

    def kernel(*refs):
        shard_ref, gate_ref, up_ref = refs[:3]
        here = lax.axis_index(axis)
        at = pl.multiple_of(lax.rem(here + step + n, n) * cols, cols)
        block = shard_ref[...]
        got = []
        for i, weight in enumerate((gate_ref, up_ref)):
            part = jnp.dot(block, weight[pl.ds(at, cols), :], preferred_element_type=jnp.float32)
            got.append(part if first else refs[3 + i][...] + part)
        if last:
            hidden = (jax.nn.silu(got[0]) * got[1]).astype(jnp.bfloat16)
            for i in range(n):
                refs[-1][i] = hidden
        else:
            refs[-2][...], refs[-1][...] = got

    sum_out = [pltpu.VMEM((rows, hid), jnp.float32)] * 2
    return pl.pallas_call(
        kernel,
        out_shape=jax.ShapeDtypeStruct((n, rows, hid), jnp.bfloat16) if last else sum_out,
        in_specs=[vmem()] * (3 if first else 5),
        out_specs=vmem() if last else [vmem()] * 2,
        name="gate_up_step",
        compiler_params=SMALL,
    )(*(in_vmem(x) for x in (shard, gate, up, *(sums or ()))))


def routing(expert_ids, gate_codes, experts, capacity):
    window = jnp.arange(experts, dtype=jnp.int32)
    hits = expert_ids[..., None] == window
    member = jnp.any(hits, axis=-2)
    codes = gate_codes.astype(jnp.float32)
    gates = 2.5 * codes / jnp.sum(codes, axis=-1, keepdims=True)
    weight = jnp.sum(jnp.where(hits, gates[..., None], jnp.float32(0.0)), axis=-2)
    tokens = expert_ids.shape[0]
    before = jnp.tril(jnp.ones((tokens, tokens), jnp.bfloat16), -1)
    rank = jnp.dot(before, member.astype(jnp.bfloat16), preferred_element_type=jnp.float32)
    slots = jnp.arange(capacity, dtype=jnp.float32)
    place = member[..., None] & (rank[..., None] == slots)
    return place, weight


def around(shard, axis):
    n = lax.axis_size(axis)
    up = [(i, (i + 1) % n) for i in range(n)]
    down = [(i, (i - 1) % n) for i in range(n)]
    found = [(0, shard)]
    a = b = shard
    for k in range(1, n // 2 + 1):
        a = lax.ppermute(a, axis, up)
        found.append((-k, a))
        if 2 * k < n:
            b = lax.ppermute(b, axis, down)
            found.append((k, b))
    return found


def per_device(tokens, expert_ids, gate_codes, w_gate, w_up, w_down):
    ny, nh = lax.axis_size("y"), lax.axis_size("xh")
    experts = lax.axis_size(EXPERT)
    own, width = tokens.shape[1], tokens.shape[2]
    cols = width // ny

    toks = exchange(in_columns(tokens[0], ny, nh), GROUP)
    own_block, *blocks = cut_blocks(w_down[0])
    sides = lax.axis_size("dp")
    for k in range(1, ny // 2 + 1):
        pairs = []
        for i in range(ny):
            for side in range(sides):
                away = k if (side == 0) == (k != 3) else -k
                pairs.append((i * sides + side, (i + away) % ny * sides + side))
        blocks[k - 1] = lax.ppermute(blocks[k - 1], ("y", "dp"), pairs)
    mine = stacked(blocks)
    others = lax.ppermute(mine, "dp", [(0, 1), (1, 0)])

    place, weight = routing(expert_ids[0], gate_codes[0], experts, CAPG)
    mix = jnp.where(place, weight[..., None], jnp.float32(0.0))
    rows = jnp.einsum(
        "tej,td->ejd",
        place.astype(jnp.bfloat16),
        toks.reshape(ny * nh * own, cols),
        preferred_element_type=jnp.float32,
    ).astype(jnp.bfloat16)
    got = exchange(rows, EXPERT)
    sets = got.shape[0]
    count = sets * CAPG
    sums = None
    shards = around(got.reshape(count, cols), "y")
    for step, shard in shards:
        last = shard is shards[-1][1]
        sums = gate_up_step(sums, shard, w_gate[0], w_up[0], step, "y", last)
    hiddens = exchange(sums, "y")
    outs = down_product(hiddens, own_block, mine, others)
    back = exchange(outs.reshape(sets, CAPG, cols), EXPERT)
    mixed = jnp.einsum(
        "tej,ejc->tc",
        mix,
        back.astype(jnp.float32),
        precision=lax.Precision.HIGHEST,
        preferred_element_type=jnp.float32,
    )
    home = exchange(mixed.astype(jnp.bfloat16).reshape(ny * nh, own, cols), GROUP)
    home = home.reshape(ny, nh, own, cols).astype(jnp.float32)
    home = jnp.sum(home, axis=1).astype(jnp.bfloat16)
    return jnp.concatenate([home[i] for i in range(ny)], axis=1)[None]


def solution(mesh):
    fine = Mesh(
        mesh.devices.reshape(8, 2, 16, 2, mesh.shape["dp"]), ("y", "xh", "z", "core", "dp")
    )
    placed = (
        P(SETS_OVER, GROUP, None),
        P(SETS_OVER, None, None),
        P(SETS_OVER, None, None),
        P(EXPERT, None, GROUP),
        P(EXPERT, None, GROUP),
        P(EXPERT, GROUP, None),
    )
    return jax.shard_map(
        per_device,
        mesh=fine,
        in_specs=placed,
        out_specs=P(SETS_OVER, GROUP, None),
        check_vma=False,
    )
```

```python
import jax
import jax.numpy as jnp
from jax import lax
from jax.experimental import pallas as pl
from jax.experimental.pallas import tpu as pltpu
from jax.sharding import Mesh
from jax.sharding import PartitionSpec as P


CAPG = 4
GROUP = ("y", "xh")
EXPERT = ("z", "core")
SETS_OVER = ("z", "core", "dp")


def exchange(parts, axes):
    return lax.all_to_all(parts, axes, 0, 0, tiled=True)


SMALL = pltpu.CompilerParams(vmem_limit_bytes=8 * 2**20)


def vmem():
    return pl.BlockSpec(memory_space=pltpu.VMEM)


def in_vmem(x):
    return pltpu.with_memory_space_constraint(x, pltpu.VMEM)


def anywhere():
    return pl.BlockSpec(memory_space=pl.ANY)


def in_columns(rows, pieces, copies):
    own, width = rows.shape
    cols = width // pieces

    def kernel(rows_ref, out_ref):
        for i in range(pieces):
            piece = rows_ref[:, i * cols : (i + 1) * cols]
            for j in range(copies):
                out_ref[i * copies + j] = piece

    return pl.pallas_call(
        kernel,
        out_shape=jax.ShapeDtypeStruct((pieces * copies, own, cols), rows.dtype),
        in_specs=[vmem()],
        out_specs=vmem(),
        name="in_columns",
        compiler_params=SMALL,
    )(rows)


def signed(k):
    here, side = lax.axis_index("y"), lax.axis_index("dp")
    away = 1 - 2 * side if k < 3 else 2 * side - 1
    return here, side, away * k


def cut_blocks(matrix):
    n, far = lax.axis_size("y"), lax.axis_size("y") // 2
    rows, width = matrix.shape
    cols, half = width // n, rows // 2

    def kernel(matrix_ref, *refs):
        outs, sems = refs[: far + 1], refs[far + 1]
        copies = []
        for k in range(far + 1):
            here, side, step = signed(k)
            step = far if k == far else step
            at = pl.multiple_of(lax.rem(here + step + n, n) * cols, cols)
            lines = pl.ds(pl.multiple_of(side * half, half), half) if k == far else slice(None)
            source = matrix_ref.at[lines, pl.ds(at, cols)]
            copies.append(pltpu.make_async_copy(source, outs[k], sems.at[k]))
        for copy in copies:
            copy.start()
        for copy in copies:
            copy.wait()

    whole, part = pltpu.VMEM((rows, cols), matrix.dtype), pltpu.VMEM((half, cols), matrix.dtype)
    return pl.pallas_call(
        kernel,
        out_shape=[whole] * far + [part],
        in_specs=[anywhere()],
        out_specs=[vmem()] * (far + 1),
        scratch_shapes=[pltpu.SemaphoreType.DMA((far + 1,))],
        name="cut_blocks",
        compiler_params=SMALL,
    )(pltpu.with_memory_space_constraint(matrix, pltpu.HBM))


def stacked(parts):
    counts = [p.shape[0] for p in parts]
    total, cols = sum(counts), parts[0].shape[1]

    def kernel(*refs):
        out_ref, sems = refs[-2:]
        copies, at = [], 0
        for k, count in enumerate(counts):
            place = out_ref.at[pl.ds(at, count), :]
            copies.append(pltpu.make_async_copy(refs[k], place, sems.at[k]))
            at += count
        for copy in copies:
            copy.start()
        for copy in copies:
            copy.wait()

    return pl.pallas_call(
        kernel,
        out_shape=pltpu.VMEM((total, cols), parts[0].dtype),
        in_specs=[anywhere()] * len(parts),
        out_specs=vmem(),
        scratch_shapes=[pltpu.SemaphoreType.DMA((len(parts),))],
        name="stacked",
        compiler_params=SMALL,
    )(*(pltpu.with_memory_space_constraint(p, pltpu.HBM) for p in parts))


def down_product(hiddens, own, mine, others):
    n, far = lax.axis_size("y"), lax.axis_size("y") // 2
    rows, hid = hiddens.shape[1:]
    half, cols = hid // 2, own.shape[1]

    def kernel(hid_ref, own_ref, mine_ref, others_ref, outs_ref, far_ref):
        here, side, _ = signed(1)
        total = jnp.dot(hid_ref[here], own_ref[...], preferred_element_type=jnp.float32)
        for k in range(1, far):
            _, _, step = signed(k)
            lines = slice((k - 1) * hid, k * hid)
            for sign, ref in ((1, mine_ref), (-1, others_ref)):
                part = hid_ref[lax.rem(here - sign * step + n, n)]
                total += jnp.dot(part, ref[lines, :], preferred_element_type=jnp.float32)
        lines = slice((far - 1) * hid, (far - 1) * hid + half)
        far_ref[pl.ds(pl.multiple_of(side * half, half), half), :] = mine_ref[lines, :]
        far_ref[pl.ds(pl.multiple_of((1 - side) * half, half), half), :] = others_ref[lines, :]
        part = hid_ref[lax.rem(here + far, n)]
        total += jnp.dot(part, far_ref[...], preferred_element_type=jnp.float32)
        outs_ref[...] = total.astype(outs_ref.dtype)

    return pl.pallas_call(
        kernel,
        out_shape=jax.ShapeDtypeStruct((rows, cols), jnp.bfloat16),
        in_specs=[vmem()] * 4,
        out_specs=vmem(),
        scratch_shapes=[pltpu.VMEM((hid, cols), own.dtype)],
        name="down_product",
        compiler_params=SMALL,
    )(*(in_vmem(x) for x in (hiddens, own, mine, others)))


def gate_up_step(sums, shard, gate, up, step, axis, last):
    n = lax.axis_size(axis)
    rows, cols = shard.shape
    hid = gate.shape[1]
    first = sums is None

    def kernel(*refs):
        shard_ref, gate_ref, up_ref = refs[:3]
        here = lax.axis_index(axis)
        at = pl.multiple_of(lax.rem(here + step + n, n) * cols, cols)
        block = shard_ref[...]
        got = []
        for i, weight in enumerate((gate_ref, up_ref)):
            part = jnp.dot(block, weight[pl.ds(at, cols), :], preferred_element_type=jnp.float32)
            got.append(part if first else refs[3 + i][...] + part)
        if last:
            hidden = (jax.nn.silu(got[0]) * got[1]).astype(jnp.bfloat16)
            for i in range(n):
                refs[-1][i] = hidden
        else:
            refs[-2][...], refs[-1][...] = got

    sum_out = [pltpu.VMEM((rows, hid), jnp.float32)] * 2
    return pl.pallas_call(
        kernel,
        out_shape=jax.ShapeDtypeStruct((n, rows, hid), jnp.bfloat16) if last else sum_out,
        in_specs=[vmem()] * (3 if first else 5),
        out_specs=vmem() if last else [vmem()] * 2,
        name="gate_up_step",
        compiler_params=SMALL,
    )(*(in_vmem(x) for x in (shard, gate, up, *(sums or ()))))


def routing(expert_ids, gate_codes, window, capacity):
    hits = expert_ids[..., None] == window
    member = jnp.any(hits, axis=-2)
    codes = gate_codes.astype(jnp.float32)
    gates = 2.5 * codes / jnp.sum(codes, axis=-1, keepdims=True)
    weight = jnp.sum(jnp.where(hits, gates[..., None], jnp.float32(0.0)), axis=-2)
    tokens = expert_ids.shape[1]
    before = jnp.tril(jnp.ones((tokens, tokens), jnp.bfloat16), -1)
    rank = jnp.einsum(
        "ut,cte->cue", before, member.astype(jnp.bfloat16), preferred_element_type=jnp.float32
    )
    slots = jnp.arange(capacity, dtype=jnp.float32)
    place = member[..., None] & (rank[..., None] == slots)
    return place, weight


def around(shard, axis):
    n = lax.axis_size(axis)
    up = [(i, (i + 1) % n) for i in range(n)]
    down = [(i, (i - 1) % n) for i in range(n)]
    found = [(0, shard)]
    a = b = shard
    for k in range(1, n // 2 + 1):
        a = lax.ppermute(a, axis, up)
        found.append((-k, a))
        if 2 * k < n:
            b = lax.ppermute(b, axis, down)
            found.append((k, b))
    return found


def per_device(tokens, expert_ids, gate_codes, w_gate, w_up, w_down):
    ny, nh = lax.axis_size("y"), lax.axis_size("xh")
    nz, nc = lax.axis_size("z"), lax.axis_size("core")
    core = lax.axis_index("core")
    own, width = tokens.shape[1], tokens.shape[2]
    cols = width // ny

    mine = jnp.stack([expert_ids[0], gate_codes[0]])
    other = lax.ppermute(mine, "core", [(0, 1), (1, 0)])
    both = jnp.where(core == 0, jnp.stack([mine, other]), jnp.stack([other, mine]))
    toks = exchange(in_columns(tokens[0], ny, nh * nc), (*GROUP, "core"))
    toks = jnp.moveaxis(toks.reshape(ny * nh, nc, own, cols), 1, 0)
    own_block, *blocks = cut_blocks(w_down[0])
    sides = lax.axis_size("dp")
    for k in range(1, ny // 2 + 1):
        pairs = []
        for i in range(ny):
            for side in range(sides):
                away = k if (side == 0) == (k != 3) else -k
                pairs.append((i * sides + side, (i + away) % ny * sides + side))
        blocks[k - 1] = lax.ppermute(blocks[k - 1], ("y", "dp"), pairs)
    mine = stacked(blocks)
    others = lax.ppermute(mine, "dp", [(0, 1), (1, 0)])

    window = nc * jnp.arange(nz, dtype=jnp.int32) + core
    place, weight = routing(both[:, 0], both[:, 1], window, CAPG)
    mix = jnp.where(place, weight[..., None], jnp.float32(0.0))
    rows = jnp.einsum(
        "ctej,ctd->ecjd",
        place.astype(jnp.bfloat16),
        toks.reshape(nc, ny * nh * own, cols),
        preferred_element_type=jnp.float32,
    ).astype(jnp.bfloat16)
    got = exchange(rows, "z")
    count = nz * nc * CAPG
    sums = None
    shards = around(got.reshape(count, cols), "y")
    for step, shard in shards:
        last = shard is shards[-1][1]
        sums = gate_up_step(sums, shard, w_gate[0], w_up[0], step, "y", last)
    hiddens = exchange(sums, "y")
    outs = down_product(hiddens, own_block, mine, others)
    back = exchange(outs.reshape(nz, nc, CAPG, cols), "z")
    mixed = jnp.einsum(
        "ctej,ecjd->tcd",
        mix,
        back.astype(jnp.float32),
        precision=lax.Precision.HIGHEST,
        preferred_element_type=jnp.float32,
    )
    mixed = mixed.astype(jnp.bfloat16).reshape(ny * nh, own, nc, cols)
    mixed = jnp.moveaxis(mixed, 2, 1).reshape(ny * nh * nc, own, cols)
    home = exchange(mixed, (*GROUP, "core"))
    home = home.reshape(ny, nh * nc, own, cols).astype(jnp.float32)
    home = jnp.sum(home, axis=1).astype(jnp.bfloat16)
    return jnp.concatenate([home[i] for i in range(ny)], axis=1)[None]


def solution(mesh):
    fine = Mesh(
        mesh.devices.reshape(8, 2, 16, 2, mesh.shape["dp"]), ("y", "xh", "z", "core", "dp")
    )
    placed = (
        P(SETS_OVER, GROUP, None),
        P(SETS_OVER, None, None),
        P(SETS_OVER, None, None),
        P(EXPERT, None, GROUP),
        P(EXPERT, None, GROUP),
        P(EXPERT, GROUP, None),
    )
    return jax.shard_map(
        per_device,
        mesh=fine,
        in_specs=placed,
        out_specs=P(SETS_OVER, GROUP, None),
        check_vma=False,
    )
```

```python
import jax
import jax.numpy as jnp
from jax import lax
from jax.experimental import pallas as pl
from jax.experimental.pallas import tpu as pltpu
from jax.sharding import Mesh
from jax.sharding import PartitionSpec as P


CAPG = 4
GROUP = ("y", "xh")
EXPERT = ("z", "core")
SETS_OVER = ("z", "core", "dp")


def exchange(parts, axes):
    return lax.all_to_all(parts, axes, 0, 0, tiled=True)


SMALL = pltpu.CompilerParams(vmem_limit_bytes=8 * 2**20)


def vmem():
    return pl.BlockSpec(memory_space=pltpu.VMEM)


def in_vmem(x):
    return pltpu.with_memory_space_constraint(x, pltpu.VMEM)


def anywhere():
    return pl.BlockSpec(memory_space=pl.ANY)


def in_columns(rows, pieces, copies):
    own, width = rows.shape
    cols = width // pieces

    def kernel(rows_ref, out_ref):
        for i in range(pieces):
            piece = rows_ref[:, i * cols : (i + 1) * cols]
            for j in range(copies):
                out_ref[i * copies + j] = piece

    return pl.pallas_call(
        kernel,
        out_shape=jax.ShapeDtypeStruct((pieces * copies, own, cols), rows.dtype),
        in_specs=[vmem()],
        out_specs=vmem(),
        name="in_columns",
        compiler_params=SMALL,
    )(rows)


def signed(k):
    here, side = lax.axis_index("y"), lax.axis_index("dp")
    away = 1 - 2 * side if k < 3 else 2 * side - 1
    return here, side, away * k


def cut_blocks(matrix):
    n, far = lax.axis_size("y"), lax.axis_size("y") // 2
    rows, width = matrix.shape
    cols, half = width // n, rows // 2

    def kernel(matrix_ref, *refs):
        outs, sems = refs[: far + 1], refs[far + 1]
        copies = []
        for k in range(far + 1):
            here, side, step = signed(k)
            step = far if k == far else step
            at = pl.multiple_of(lax.rem(here + step + n, n) * cols, cols)
            lines = pl.ds(pl.multiple_of(side * half, half), half) if k == far else slice(None)
            source = matrix_ref.at[lines, pl.ds(at, cols)]
            copies.append(pltpu.make_async_copy(source, outs[k], sems.at[k]))
        for copy in copies:
            copy.start()
        for copy in copies:
            copy.wait()

    whole, part = pltpu.VMEM((rows, cols), matrix.dtype), pltpu.VMEM((half, cols), matrix.dtype)
    return pl.pallas_call(
        kernel,
        out_shape=[whole] * far + [part],
        in_specs=[anywhere()],
        out_specs=[vmem()] * (far + 1),
        scratch_shapes=[pltpu.SemaphoreType.DMA((far + 1,))],
        name="cut_blocks",
        compiler_params=SMALL,
    )(pltpu.with_memory_space_constraint(matrix, pltpu.HBM))


def stacked(parts):
    counts = [p.shape[0] for p in parts]
    total, cols = sum(counts), parts[0].shape[1]

    def kernel(*refs):
        out_ref, sems = refs[-2:]
        copies, at = [], 0
        for k, count in enumerate(counts):
            place = out_ref.at[pl.ds(at, count), :]
            copies.append(pltpu.make_async_copy(refs[k], place, sems.at[k]))
            at += count
        for copy in copies:
            copy.start()
        for copy in copies:
            copy.wait()

    return pl.pallas_call(
        kernel,
        out_shape=pltpu.VMEM((total, cols), parts[0].dtype),
        in_specs=[anywhere()] * len(parts),
        out_specs=vmem(),
        scratch_shapes=[pltpu.SemaphoreType.DMA((len(parts),))],
        name="stacked",
        compiler_params=SMALL,
    )(*(pltpu.with_memory_space_constraint(p, pltpu.HBM) for p in parts))


def down_product(hiddens, own, mine, others):
    n, far = lax.axis_size("y"), lax.axis_size("y") // 2
    rows, hid = hiddens.shape[1:]
    half, cols = hid // 2, own.shape[1]

    def kernel(hid_ref, own_ref, mine_ref, others_ref, outs_ref, far_ref):
        here, side, _ = signed(1)
        total = jnp.dot(hid_ref[here], own_ref[...], preferred_element_type=jnp.float32)
        for k in range(1, far):
            _, _, step = signed(k)
            lines = slice((k - 1) * hid, k * hid)
            for sign, ref in ((1, mine_ref), (-1, others_ref)):
                part = hid_ref[lax.rem(here - sign * step + n, n)]
                total += jnp.dot(part, ref[lines, :], preferred_element_type=jnp.float32)
        lines = slice((far - 1) * hid, (far - 1) * hid + half)
        far_ref[pl.ds(pl.multiple_of(side * half, half), half), :] = mine_ref[lines, :]
        far_ref[pl.ds(pl.multiple_of((1 - side) * half, half), half), :] = others_ref[lines, :]
        part = hid_ref[lax.rem(here + far, n)]
        total += jnp.dot(part, far_ref[...], preferred_element_type=jnp.float32)
        outs_ref[...] = total.astype(outs_ref.dtype)

    return pl.pallas_call(
        kernel,
        out_shape=jax.ShapeDtypeStruct((rows, cols), jnp.bfloat16),
        in_specs=[vmem()] * 4,
        out_specs=vmem(),
        scratch_shapes=[pltpu.VMEM((hid, cols), own.dtype)],
        name="down_product",
        compiler_params=SMALL,
    )(*(in_vmem(x) for x in (hiddens, own, mine, others)))


def gate_up_step(sums, shard, gate, up, step, axis, last):
    n = lax.axis_size(axis)
    rows, cols = shard.shape
    hid = gate.shape[1]
    first = sums is None

    def kernel(*refs):
        shard_ref, gate_ref, up_ref = refs[:3]
        here = lax.axis_index(axis)
        at = pl.multiple_of(lax.rem(here + step + n, n) * cols, cols)
        block = shard_ref[...]
        got = []
        for i, weight in enumerate((gate_ref, up_ref)):
            part = jnp.dot(block, weight[pl.ds(at, cols), :], preferred_element_type=jnp.float32)
            got.append(part if first else refs[3 + i][...] + part)
        if last:
            hidden = (jax.nn.silu(got[0]) * got[1]).astype(jnp.bfloat16)
            for i in range(n):
                refs[-1][i] = hidden
        else:
            refs[-2][...], refs[-1][...] = got

    sum_out = [pltpu.VMEM((rows, hid), jnp.float32)] * 2
    return pl.pallas_call(
        kernel,
        out_shape=jax.ShapeDtypeStruct((n, rows, hid), jnp.bfloat16) if last else sum_out,
        in_specs=[vmem()] * (3 if first else 5),
        out_specs=vmem() if last else [vmem()] * 2,
        name="gate_up_step",
        compiler_params=SMALL,
    )(*(in_vmem(x) for x in (shard, gate, up, *(sums or ()))))


def routing(expert_ids, gate_codes, window, capacity):
    hits = expert_ids[..., None] == window
    member = jnp.any(hits, axis=-2)
    codes = gate_codes.astype(jnp.float32)
    gates = 2.5 * codes / jnp.sum(codes, axis=-1, keepdims=True)
    weight = jnp.sum(jnp.where(hits, gates[..., None], jnp.float32(0.0)), axis=-2)
    tokens = expert_ids.shape[1]
    before = jnp.tril(jnp.ones((tokens, tokens), jnp.float32), -1)
    rank = jnp.einsum("ut,cte->cue", before, member.astype(jnp.float32))
    slots = jnp.arange(capacity, dtype=jnp.float32)
    place = member[..., None] & (rank[..., None] == slots)
    return place, weight


def around(shard, axis):
    n = lax.axis_size(axis)
    up = [(i, (i + 1) % n) for i in range(n)]
    down = [(i, (i - 1) % n) for i in range(n)]
    found = [(0, shard)]
    a = b = shard
    for k in range(1, n // 2 + 1):
        a = lax.ppermute(a, axis, up)
        found.append((-k, a))
        if 2 * k < n:
            b = lax.ppermute(b, axis, down)
            found.append((k, b))
    return found


def per_device(tokens, expert_ids, gate_codes, w_gate, w_up, w_down):
    ny, nh = lax.axis_size("y"), lax.axis_size("xh")
    nz, nc = lax.axis_size("z"), lax.axis_size("core")
    core = lax.axis_index("core")
    own, width = tokens.shape[1], tokens.shape[2]
    cols = width // ny

    mine = jnp.stack([expert_ids[0], gate_codes[0]])
    other = lax.ppermute(mine, "core", [(0, 1), (1, 0)])
    both = jnp.where(core == 0, jnp.stack([mine, other]), jnp.stack([other, mine]))
    toks = exchange(in_columns(tokens[0], ny, nh), GROUP)
    own_block, *blocks = cut_blocks(w_down[0])
    sides = lax.axis_size("dp")
    for k in range(1, ny // 2 + 1):
        pairs = []
        for i in range(ny):
            for side in range(sides):
                away = k if (side == 0) == (k != 3) else -k
                pairs.append((i * sides + side, (i + away) % ny * sides + side))
        blocks[k - 1] = lax.ppermute(blocks[k - 1], ("y", "dp"), pairs)
    mine = stacked(blocks)
    others = lax.ppermute(mine, "dp", [(0, 1), (1, 0)])

    experts = jnp.arange(nz * nc, dtype=jnp.int32)
    place, _ = routing(expert_ids, gate_codes, experts, CAPG)
    rows = jnp.einsum(
        "tej,td->ejd",
        place[0].astype(jnp.bfloat16),
        toks.reshape(ny * nh * own, cols),
        preferred_element_type=jnp.float32,
    ).astype(jnp.bfloat16)
    got = exchange(rows, EXPERT)
    window = nc * jnp.arange(nz, dtype=jnp.int32) + core
    place, weight = routing(both[:, 0], both[:, 1], window, CAPG)
    mix = jnp.where(place, weight[..., None], jnp.float32(0.0))
    count = nz * nc * CAPG
    sums = None
    shards = around(got.reshape(count, cols), "y")
    for step, shard in shards:
        last = shard is shards[-1][1]
        sums = gate_up_step(sums, shard, w_gate[0], w_up[0], step, "y", last)
    hiddens = exchange(sums, "y")
    outs = down_product(hiddens, own_block, mine, others)
    back = exchange(outs.reshape(nz, nc, CAPG, cols), "z")
    mixed = jnp.einsum(
        "ctej,ecjd->tcd",
        mix,
        back.astype(jnp.float32),
        precision=lax.Precision.HIGHEST,
        preferred_element_type=jnp.float32,
    )
    mixed = mixed.astype(jnp.bfloat16).reshape(ny * nh, own, nc, cols)
    mixed = jnp.moveaxis(mixed, 2, 1).reshape(ny * nh * nc, own, cols)
    home = exchange(mixed, (*GROUP, "core"))
    home = home.reshape(ny, nh * nc, own, cols).astype(jnp.float32)
    home = jnp.sum(home, axis=1).astype(jnp.bfloat16)
    return jnp.concatenate([home[i] for i in range(ny)], axis=1)[None]


def solution(mesh):
    fine = Mesh(
        mesh.devices.reshape(8, 2, 16, 2, mesh.shape["dp"]), ("y", "xh", "z", "core", "dp")
    )
    placed = (
        P(SETS_OVER, GROUP, None),
        P(SETS_OVER, None, None),
        P(SETS_OVER, None, None),
        P(EXPERT, None, GROUP),
        P(EXPERT, None, GROUP),
        P(EXPERT, GROUP, None),
    )
    return jax.shard_map(
        per_device,
        mesh=fine,
        in_specs=placed,
        out_specs=P(SETS_OVER, GROUP, None),
        check_vma=False,
    )
```
